32 devices in a mesh: dp: 2 (over y), ctx: 8 (over z, x), tp: 2 (over core).
Axes of the slice: x: 2, y: 2, z: 4, core: 2. Of those that a mesh axis runs over, the one named last changes fastest.
Arguments:
- queries: bfloat16 [4, 1024, 4096], P('dp', 'ctx', 'tp'), may hold values from -6 to 6
- keys: bfloat16 [4, 1024, 512], P('dp', 'ctx', 'tp'), may hold values from -6 to 6
- values: bfloat16 [4, 1024, 512], P('dp', 'ctx', 'tp'), may hold values from -6 to 6
- output_gradient: bfloat16 [4, 1024, 4096], P('dp', 'ctx', 'tp'), may hold values from -6 to 6
- sinks: float32 [64], P('tp'), may hold values from -1 to 3
- doc_starts: int32 [4, 64], P('dp'), may hold values from 0 to 2048, as said below
- valid_counts: int32 [4, 8], P('dp'), may hold values from 64 to 128
Outputs:
- query_grad: bfloat16 [4, 1024, 4096], P('dp', 'ctx', 'tp')
- key_grad: bfloat16 [4, 1024, 512], P('dp', 'ctx', 'tp')
- value_grad: bfloat16 [4, 1024, 512], P('dp', 'ctx', 'tp')
- sink_grad: float32 [64], P('tp')
The draws below stay inside these ranges and needn't reach their ends.
Inputs may be any that keep to these rules, and one draw needn't show every extreme that they name: `doc_starts`: each row is strictly increasing, begins with 0 and ends with 2048; a start at or past 1024 opens no document.
All inputs are finite; a program needn't handle non-finite values.
Results may differ from the reference program's by a relative error of at most 0.0093.
Values may be sent and summed in bfloat16 or wider, within the bound.
No kernel may reach another device: no remote copies, remote signals or barrier semaphores. Data moves between devices by JAX's collectives and lax.ppermute only.
A program may use at most 64 MiB of HBM per device.

```python
import jax
import jax.numpy as jnp
from jax import lax

QUERY_HEADS = 64
KEY_VALUE_HEADS = 8
HEAD_DIMENSION = 64
WINDOW_LENGTH = 128
CTX_TOK = 128
DOCS = 64
SEQUENCE_LENGTH = 1024
BATCH_SEQUENCES = 4
N_CTX = 8


def draw_queries(key, part):
    regular_portion = jax.random.normal(jax.random.fold_in(key, 1), (BATCH_SEQUENCES, SEQUENCE_LENGTH, QUERY_HEADS * HEAD_DIMENSION), jnp.float32)
    result = jnp.clip(regular_portion, -6.0, 6.0)
    return result.astype(jnp.bfloat16)


def draw_keys(key, part):
    regular_portion = jax.random.normal(jax.random.fold_in(key, 2), (BATCH_SEQUENCES, SEQUENCE_LENGTH, KEY_VALUE_HEADS * HEAD_DIMENSION), jnp.float32)
    result = jnp.clip(regular_portion, -6.0, 6.0)
    return result.astype(jnp.bfloat16)


def draw_doc_starts(key, part):
    spacing = jax.random.randint(jax.random.fold_in(key, 3), (BATCH_SEQUENCES, DOCS), 1, 2 * SEQUENCE_LENGTH // DOCS)
    running = jnp.cumsum(spacing, axis=1)
    starts = (running - spacing[:, :1]).astype(jnp.int32)
    last_column = jnp.arange(DOCS, dtype=jnp.int32)[None, :] == DOCS - 1
    return jnp.where(last_column, jnp.int32(2 * SEQUENCE_LENGTH), starts).astype(jnp.int32)


def place_ends(values, stream_key, least, top_value):
    longest = values.shape.index(max(values.shape))
    spots = []
    for shift in (0, 1):
        where = [jax.random.randint(jax.random.fold_in(stream_key, axis), (), 0, length) for axis, length in enumerate(values.shape)]
        where[longest] = (where[longest] + shift) % values.shape[longest]
        spots.append(tuple(where))
    return values.at[spots[0]].set(least).at[spots[1]].set(top_value)


def level_of(own_key, extent, cuts, low, top_value):
    loudness, own = 1.0, jax.random.fold_in(own_key, 6)
    for dim, shards_of in cuts:
        heights = jnp.exp(jax.random.uniform(jax.random.fold_in(own, dim), (shards_of,), jnp.float32, low / len(cuts), top_value / len(cuts)))
        loudness = loudness * jnp.repeat(heights, extent[dim] // shards_of).reshape([-1 if axis == dim else 1 for axis in range(len(extent))])
    return loudness


def normal_values(rng, dims, width, reach, shards=(), held_as=jnp.bfloat16):
    drawn = jax.random.normal(rng, dims, jnp.float32) * width
    if len(shards) > 0:
        drawn = level_of(rng, dims, shards, -0.22, 0.18) * drawn
    return jnp.clip(drawn, min=-reach, max=reach).astype(held_as)


def setup_inputs(seed: int = 0) -> dict:
    seeds = jax.random.split(jax.random.key(seed), 8)
    queries = draw_queries(jax.random.fold_in(seeds[7], 71), 0)
    keys = draw_keys(jax.random.fold_in(seeds[7], 71), 0)
    values = normal_values(seeds[2], (BATCH_SEQUENCES, SEQUENCE_LENGTH, KEY_VALUE_HEADS * HEAD_DIMENSION), 1.0, 6.0, ((0, 2), (1, 8), (2, 2)))
    output_gradient = normal_values(seeds[3], (BATCH_SEQUENCES, SEQUENCE_LENGTH, QUERY_HEADS * HEAD_DIMENSION), 1.0, 6.0, ((0, 2), (1, 8), (2, 2)))
    sinks = jnp.clip(-1.0 + 4.0 * jax.random.uniform(seeds[4], (QUERY_HEADS,), jnp.float32) ** level_of(seeds[4], (QUERY_HEADS,), ((0, 2),), -0.2, 0.2), -1.0, 3.0)
    doc_starts = draw_doc_starts(jax.random.fold_in(seeds[7], 71), 0)
    valid_counts = place_ends(jax.random.randint(seeds[6], (BATCH_SEQUENCES, N_CTX), CTX_TOK - WINDOW_LENGTH // 2, CTX_TOK + 1), jax.random.fold_in(seeds[6], 1), CTX_TOK - WINDOW_LENGTH // 2, CTX_TOK).astype(jnp.int32)
    return dict(queries=queries, keys=keys, values=values, output_gradient=output_gradient, sinks=sinks, doc_starts=doc_starts, valid_counts=valid_counts)


masked_score = -1e30


def document_ids(starts, positions):
    return jnp.sum((starts[None, :] <= positions[:, None]).astype(jnp.int32), axis=1)


def key_valid_mask(counts, positions, block_rows):
    block_index = positions // block_rows
    offset = positions - block_index * block_rows
    matches = jnp.arange(counts.shape[0], dtype=jnp.int32)[None, :] == block_index[:, None]
    limits = jnp.sum(jnp.where(matches, counts[None, :], 0), axis=1)
    return offset < limits


def band_grads(query_tile_block, key_tile_block, value_tile_block, output_grad_block, query_pos, key_pos, query_doc, key_doc, key_valid, sink_logits):
    heads_kv = key_tile_block.shape[2]
    query_group_width = query_tile_block.shape[3]
    scaling = query_tile_block.shape[4] ** -0.5
    query_wide = query_tile_block.astype(jnp.float32)
    key_wide = key_tile_block.astype(jnp.float32)
    value_wide = value_tile_block.astype(jnp.float32)
    grad_wide = output_grad_block.astype(jnp.float32)
    scores = jnp.einsum('nqhgd,nkhd->nhgqk', query_wide, key_wide) * scaling
    allowed = (key_pos[:, None, :] <= query_pos[:, :, None]) & (query_pos[:, :, None] - key_pos[:, None, :] < WINDOW_LENGTH)
    allowed = allowed & (query_doc[:, :, None] == key_doc[:, None, :]) & key_valid[:, None, :]
    scores = jnp.where(allowed[:, None, None], scores, masked_score)
    sink_term = sink_logits.reshape(heads_kv, query_group_width)[None, :, :, None]
    maxima = jnp.maximum(jnp.max(scores, axis=-1), sink_term)
    powers = jnp.exp(scores - maxima[..., None])
    sink_exp = jnp.exp(sink_term - maxima)
    denominator = jnp.sum(powers, axis=-1) + sink_exp
    attend = powers / denominator[..., None]
    attend_low = lax.optimization_barrier(attend.astype(jnp.bfloat16)).astype(jnp.float32)
    context = jnp.einsum('nhgqk,nkhd->nhgqd', attend_low, value_wide)
    deltas = jnp.sum(jnp.transpose(grad_wide, (0, 2, 3, 1, 4)) * context, axis=-1)
    grad_attend = jnp.einsum('nqhgd,nkhd->nhgqk', grad_wide, value_wide)
    grad_score = attend * (grad_attend - deltas[..., None])
    score_low = lax.optimization_barrier(grad_score.astype(jnp.bfloat16)).astype(jnp.float32)
    query_grad = jnp.einsum('nhgqk,nkhd->nqhgd', score_low, key_wide) * scaling
    key_grad = jnp.einsum('nhgqk,nqhgd->nkhd', score_low, query_wide) * scaling
    value_grad = jnp.einsum('nhgqk,nqhgd->nkhd', attend_low, grad_wide)
    sink_grad = -jnp.sum(sink_exp / denominator * deltas, axis=-1)
    return query_grad, key_grad, value_grad, sink_grad.reshape(sink_grad.shape[0], heads_kv * query_group_width)


def paired_block_tiles(sequence_rows, block_tiles, heads_kv):
    padded = jnp.concatenate([jnp.zeros((WINDOW_LENGTH, heads_kv * HEAD_DIMENSION), sequence_rows.dtype), sequence_rows], axis=0)
    padded = padded.reshape(block_tiles + 1, WINDOW_LENGTH, heads_kv, HEAD_DIMENSION)
    return jnp.concatenate([padded[:-1], padded[1:]], axis=1)


def reference(queries, keys, values, output_gradient, sinks, doc_starts, valid_counts):
    block_tiles = SEQUENCE_LENGTH // WINDOW_LENGTH
    query_group_width = QUERY_HEADS // KEY_VALUE_HEADS
    query_lines = jnp.arange(SEQUENCE_LENGTH, dtype=jnp.int32).reshape(block_tiles, WINDOW_LENGTH)
    key_lines = jnp.arange(-WINDOW_LENGTH, SEQUENCE_LENGTH, dtype=jnp.int32).reshape(block_tiles + 1, WINDOW_LENGTH)
    key_lines = jnp.concatenate([key_lines[:-1], key_lines[1:]], axis=1)
    query_list = []
    key_block_items = []
    value_block_items = []
    sink_total = jnp.zeros((QUERY_HEADS,), jnp.float32)
    for sequence_index in range(BATCH_SEQUENCES):
        query_doc = document_ids(doc_starts[sequence_index], query_lines.reshape(-1)).reshape(block_tiles, WINDOW_LENGTH)
        key_doc = document_ids(doc_starts[sequence_index], key_lines.reshape(-1)).reshape(block_tiles, 2 * WINDOW_LENGTH)
        key_valid = key_valid_mask(valid_counts[sequence_index], key_lines.reshape(-1), CTX_TOK).reshape(block_tiles, 2 * WINDOW_LENGTH)
        query_tile_block = queries[sequence_index].reshape(block_tiles, WINDOW_LENGTH, KEY_VALUE_HEADS, query_group_width, HEAD_DIMENSION)
        output_grad_block = output_gradient[sequence_index].reshape(block_tiles, WINDOW_LENGTH, KEY_VALUE_HEADS, query_group_width, HEAD_DIMENSION)
        key_tile_block = paired_block_tiles(keys[sequence_index], block_tiles, KEY_VALUE_HEADS)
        value_tile_block = paired_block_tiles(values[sequence_index], block_tiles, KEY_VALUE_HEADS)

        def per_block(entries):
            results = band_grads(*[member[None] for member in entries], sinks)
            return tuple(member[0] for member in results)

        dq_all, dk_all, dv_all, sink_part = lax.map(per_block, (query_tile_block, key_tile_block, value_tile_block, output_grad_block, query_lines, key_lines, query_doc, key_doc, key_valid))
        key_grad_overall = dk_all[:, WINDOW_LENGTH:] + jnp.concatenate([dk_all[1:, :WINDOW_LENGTH], jnp.zeros_like(dk_all[:1, :WINDOW_LENGTH])], axis=0)
        value_grad_overall = dv_all[:, WINDOW_LENGTH:] + jnp.concatenate([dv_all[1:, :WINDOW_LENGTH], jnp.zeros_like(dv_all[:1, :WINDOW_LENGTH])], axis=0)
        query_list.append(dq_all.reshape(SEQUENCE_LENGTH, QUERY_HEADS * HEAD_DIMENSION).astype(jnp.bfloat16))
        key_block_items.append(key_grad_overall.reshape(SEQUENCE_LENGTH, KEY_VALUE_HEADS * HEAD_DIMENSION).astype(jnp.bfloat16))
        value_block_items.append(value_grad_overall.reshape(SEQUENCE_LENGTH, KEY_VALUE_HEADS * HEAD_DIMENSION).astype(jnp.bfloat16))
        sink_total = sink_total + jnp.sum(sink_part, axis=0)
    return (jnp.stack(query_list), jnp.stack(key_block_items), jnp.stack(value_block_items), sink_total)
```

```python
import functools
import math

import jax
import jax.numpy as jnp
from jax import lax
from jax.experimental import pallas as pl
from jax.experimental.pallas import tpu as pltpu
from jax.sharding import PartitionSpec as P

HEAD_DIMENSION = 64
WINDOW_LENGTH = 128
LANES = 128

masked_score = -1e30

dot_nt = functools.partial(
    lax.dot_general,
    dimension_numbers=(((1,), (1,)), ((), ())),
    preferred_element_type=jnp.float32,
)
dot_nn = functools.partial(
    lax.dot_general,
    dimension_numbers=(((1,), (0,)), ((), ())),
    preferred_element_type=jnp.float32,
)


def passed_along(value, axis, steps):
    count = lax.axis_size(axis)
    first, last = (max(0, -steps), min(count, count - steps))
    return lax.ppermute(value, axis, [(source, source + steps) for source in range(first, last)])


def total_over(value, axes):
    for axis in axes:
        count = lax.axis_size(axis)
        if count & (count - 1):
            value = lax.psum(value, axis)
            continue
        step = 1
        while step < count:
            value = value + lax.ppermute(value, axis, [(i, i ^ step) for i in range(count)])
            step *= 2
    return value


def lane_half():
    return lax.broadcasted_iota(jnp.int32, (WINDOW_LENGTH, LANES), 1) < HEAD_DIMENSION


def half_pair(tile, which):
    low = lane_half()
    wide = tile.astype(jnp.float32)
    if which == 0:
        lo = jnp.where(low, wide, 0.0)
        hi = pltpu.roll(lo, HEAD_DIMENSION, 1)
    else:
        hi = jnp.where(low, 0.0, wide)
        lo = pltpu.roll(hi, HEAD_DIMENSION, 1)
    return lo.astype(jnp.bfloat16), hi.astype(jnp.bfloat16)


def write_masks(starts_ref, counts_ref, seq, block, own_bias, prev_bias):
    base = block * WINDOW_LENGTH
    query = base + lax.broadcasted_iota(jnp.int32, (8, LANES), 1)
    oldest = jnp.zeros((8, LANES), jnp.int32)
    for entry in range(starts_ref.shape[1]):
        start = starts_ref[seq, entry]
        oldest = jnp.maximum(oldest, jnp.where(start <= query, start, 0))
    oldest = jnp.broadcast_to(oldest[:1], (WINDOW_LENGTH, LANES))
    key_row = lax.broadcasted_iota(jnp.int32, (WINDOW_LENGTH, LANES), 0)
    query_lane = lax.broadcasted_iota(jnp.int32, (WINDOW_LENGTH, LANES), 1)
    own_limit = counts_ref[seq, block]
    prev_limit = counts_ref[seq, jnp.maximum(block - 1, 0)]
    own = (key_row <= query_lane) & (key_row + base >= oldest) & (key_row < own_limit)
    prev = (
        (key_row > query_lane)
        & (key_row + (base - WINDOW_LENGTH) >= oldest)
        & (key_row < prev_limit)
    )
    own_bias[...] = jnp.where(own, 0.0, masked_score)
    prev_bias[...] = jnp.where(prev, 0.0, masked_score)


def twice(tile):
    return jnp.concatenate([tile, tile], axis=1)


def grads_kernel(
    sinks_ref,
    starts_ref,
    counts_ref,
    q_ref,
    g_ref,
    k_ref,
    v_ref,
    hk_ref,
    hv_ref,
    dq_ref,
    own_ref,
    prev_ref,
    sink_ref,
    own_bias,
    prev_bias,
    sink_rows,
    *,
    group,
):
    seq, pair = pl.program_id(0), pl.program_id(1)
    pairs = pl.num_programs(1)
    block = lax.axis_index("ctx")
    scaling = HEAD_DIMENSION**-0.5
    to_exp2 = scaling * math.log2(math.e)

    @pl.when(pair == 0)
    def _():
        write_masks(starts_ref, counts_ref, seq, block, own_bias, prev_bias)

    @pl.when((seq == 0) & (pair == 0))
    def _():
        sink_rows[...] = jnp.zeros_like(sink_rows)

    bias_own, bias_prev = twice(own_bias[...]), twice(prev_bias[...])
    key_row = lax.broadcasted_iota(jnp.int32, (WINDOW_LENGTH, 2 * LANES), 0)
    query_lane = lax.broadcasted_iota(jnp.int32, (WINDOW_LENGTH, 2 * LANES), 1) % LANES
    lower = key_row <= query_lane
    lower_low = lower.astype(jnp.float32).astype(jnp.bfloat16)
    first_head = lax.broadcasted_iota(jnp.int32, (1, 2 * LANES), 1) < LANES
    low = jnp.concatenate([lane_half(), lane_half()], axis=0)

    k_own, v_own = k_ref[0], v_ref[0]
    k_prev, v_prev = hk_ref[0], hv_ref[0]
    kt_own, kt_prev = k_own.T, k_prev.T
    sums = []
    for which in range(2):
        keys = jnp.concatenate(
            [*half_pair(k_own, which), *half_pair(k_prev, which)], axis=0
        )
        vals = jnp.concatenate(
            [*half_pair(v_own, which), *half_pair(v_prev, which)], axis=0
        )
        rows = slice(which * HEAD_DIMENSION, (which + 1) * HEAD_DIMENSION)
        keys_t = jnp.concatenate([kt_own[rows], kt_prev[rows]], axis=1)
        totals = [[[], []], [[], []]]
        for quad in range(group // 4):
            at = (which * group + quad * 4) * HEAD_DIMENSION
            spans = (slice(at, at + LANES), slice(at + LANES, at + 2 * LANES))
            q_cat = jnp.concatenate([q_ref[0, :, span] for span in spans], axis=0)
            g_cat = jnp.concatenate([g_ref[0, :, span] for span in spans], axis=0)
            scores = dot_nt(keys, q_cat)
            dprobs = dot_nt(vals, g_cat)
            dq_parts = []
            for half in range(2):
                own_rows = slice(half * WINDOW_LENGTH, (half + 1) * WINDOW_LENGTH)
                prev_rows = slice((half + 2) * WINDOW_LENGTH, (half + 3) * WINDOW_LENGTH)
                head = pair * 2 * group + which * group + quad * 4 + half
                sink = jnp.where(first_head, sinks_ref[head], sinks_ref[head + 2]) / scaling
                s = jnp.maximum(scores[own_rows] + bias_own, scores[prev_rows] + bias_prev)
                top = jnp.maximum(jnp.max(s, axis=0, keepdims=True), sink)
                power = jnp.exp2((s - top) * to_exp2)
                sink_power = jnp.exp2((sink - top) * to_exp2)
                inverse = 1.0 / (jnp.sum(power, axis=0, keepdims=True) + sink_power)
                dprob = jnp.where(lower, dprobs[own_rows], dprobs[prev_rows])
                delta = jnp.sum(power * dprob, axis=0, keepdims=True) * inverse
                prob = power * inverse
                dscore = prob * (dprob - delta)
                sink_term = sink_power * inverse * delta
                sink_rows[pl.ds(head, 1), :] += sink_term[:, :LANES]
                sink_rows[pl.ds(head + 2, 1), :] += sink_term[:, LANES:]
                prob_low = prob.astype(jnp.bfloat16)
                dscore_low = dscore.astype(jnp.bfloat16)
                prob_own = prob_low * lower_low
                dscore_own = dscore_low * lower_low
                prob_both = jnp.concatenate([prob_own, prob_low - prob_own], axis=0)
                dscore_both = jnp.concatenate([dscore_own, dscore_low - dscore_own], axis=0)
                dq_parts.append(dot_nn(keys_t, dscore_both) * scaling)
                totals[0][half].append((dscore_both, q_cat))
                totals[1][half].append((prob_both, g_cat))
            for part in range(2):
                lanes = slice(part * LANES, (part + 1) * LANES)
                tile = jnp.concatenate([dq_parts[0][:, lanes], dq_parts[1][:, lanes]], axis=0)
                dq_ref[0, :, spans[part]] = tile.astype(jnp.bfloat16).T
        sums.append(
            [
                [
                    dot_nn(
                        jnp.concatenate([left for left, _ in totals[kind][half]], axis=1),
                        jnp.concatenate([right for _, right in totals[kind][half]], axis=0),
                    )
                    for half in range(2)
                ]
                for kind in range(2)
            ]
        )
    for kind, factor in ((0, scaling), (1, 1.0)):
        (lo0, hi0), (lo1, hi1) = sums[0][kind], sums[1][kind]
        grad = jnp.where(low, lo0, hi1) + pltpu.roll(
            jnp.where(low, lo1, hi0), HEAD_DIMENSION, 1
        )
        grad = grad * factor
        own_ref[kind, 0] = grad[:WINDOW_LENGTH]
        prev_ref[kind, 0] = grad[WINDOW_LENGTH:].astype(jnp.bfloat16)

    @pl.when((seq == pl.num_programs(0) - 1) & (pair == pairs - 1))
    def _():
        sink_ref[...] = -jnp.sum(sink_rows[...].T, axis=0, keepdims=True)


def local(queries, keys, values, output_gradient, sinks, doc_starts, valid_counts):
    seq_count, row_count, query_width = queries.shape
    kv_width = keys.shape[2]
    heads_kv = kv_width // HEAD_DIMENSION
    head_count = sinks.shape[0]
    group = head_count // heads_kv
    pairs = heads_kv // 2
    assert row_count == WINDOW_LENGTH
    halo = passed_along(jnp.stack([keys, values]), "ctx", 1)
    wide = 2 * group * HEAD_DIMENSION
    smem = pl.BlockSpec(memory_space=pltpu.SMEM)
    wide_spec = pl.BlockSpec((1, row_count, wide), lambda b, p: (b, 0, p))
    kv_spec = pl.BlockSpec((1, row_count, LANES), lambda b, p: (b, 0, p))
    both_spec = pl.BlockSpec((2, 1, row_count, LANES), lambda b, p: (0, b, 0, p))
    padded_heads = -(-head_count // LANES) * LANES
    query_grad, own, prev, sink_part = pl.pallas_call(
        functools.partial(grads_kernel, group=group),
        grid=(seq_count, pairs),
        in_specs=[smem, smem, smem, wide_spec, wide_spec, kv_spec, kv_spec]
        + [
            pl.BlockSpec((None, 1, row_count, LANES), lambda b, p, kind=kind: (kind, b, 0, p))
            for kind in range(2)
        ],
        out_specs=[
            wide_spec,
            both_spec,
            both_spec,
            pl.BlockSpec((1, padded_heads), lambda b, p: (0, 0)),
        ],
        out_shape=[
            jax.ShapeDtypeStruct(queries.shape, jnp.bfloat16),
            jax.ShapeDtypeStruct((2,) + keys.shape, jnp.float32),
            jax.ShapeDtypeStruct((2,) + keys.shape, jnp.bfloat16),
            jax.ShapeDtypeStruct((1, padded_heads), jnp.float32),
        ],
        scratch_shapes=[
            pltpu.VMEM((WINDOW_LENGTH, LANES), jnp.float32),
            pltpu.VMEM((WINDOW_LENGTH, LANES), jnp.float32),
            pltpu.VMEM((padded_heads, LANES), jnp.float32),
        ],
    )(
        sinks,
        doc_starts,
        valid_counts,
        queries,
        output_gradient,
        keys,
        values,
        halo,
        halo,
    )
    edge = passed_along(prev, "ctx", -1)
    total = (own + edge.astype(jnp.float32)).astype(jnp.bfloat16)
    sink_grad = total_over(sink_part[0, :head_count], ("dp", "ctx"))
    return (query_grad, total[0], total[1], sink_grad)


def solution(mesh):
    placed = (
        P("dp", "ctx", "tp"),
        P("dp", "ctx", "tp"),
        P("dp", "ctx", "tp"),
        P("dp", "ctx", "tp"),
        P("tp"),
        P("dp", None),
        P("dp", None),
    )
    return jax.shard_map(
        local,
        mesh=mesh,
        in_specs=placed,
        out_specs=(P("dp", "ctx", "tp"), P("dp", "ctx", "tp"), P("dp", "ctx", "tp"), P("tp")),
        check_vma=False,
    )
```

```python
import functools
import math

import jax
import jax.numpy as jnp
from jax import lax
from jax.experimental import pallas as pl
from jax.experimental.pallas import tpu as pltpu
from jax.sharding import PartitionSpec as P

HEAD_DIMENSION = 64
WINDOW_LENGTH = 128
LANES = 128

masked_score = -1e30

dot_nt = functools.partial(
    lax.dot_general,
    dimension_numbers=(((1,), (1,)), ((), ())),
    preferred_element_type=jnp.float32,
)
dot_nn = functools.partial(
    lax.dot_general,
    dimension_numbers=(((1,), (0,)), ((), ())),
    preferred_element_type=jnp.float32,
)


def passed_along(value, axis, steps):
    count = lax.axis_size(axis)
    first, last = (max(0, -steps), min(count, count - steps))
    return lax.ppermute(value, axis, [(source, source + steps) for source in range(first, last)])


def total_over(value, axes):
    for axis in axes:
        count = lax.axis_size(axis)
        if count & (count - 1):
            value = lax.psum(value, axis)
            continue
        step = 1
        while step < count:
            value = value + lax.ppermute(value, axis, [(i, i ^ step) for i in range(count)])
            step *= 2
    return value


def lane_half(rows):
    return lax.broadcasted_iota(jnp.int32, (rows, LANES), 1) < HEAD_DIMENSION


def half_pair(tile, which):
    low = lane_half(WINDOW_LENGTH)
    wide = tile.astype(jnp.float32)
    if which == 0:
        lo = jnp.where(low, wide, 0.0)
        hi = pltpu.roll(lo, HEAD_DIMENSION, 1)
    else:
        hi = jnp.where(low, 0.0, wide)
        lo = pltpu.roll(hi, HEAD_DIMENSION, 1)
    return jnp.concatenate([lo, hi], axis=0).astype(jnp.bfloat16)


def twice(tile):
    return jnp.concatenate([tile, tile], axis=1)


def lower_triangle():
    key_row = lax.broadcasted_iota(jnp.int32, (WINDOW_LENGTH, LANES), 0)
    query_lane = lax.broadcasted_iota(jnp.int32, (WINDOW_LENGTH, LANES), 1)
    return key_row <= query_lane


def biases(starts_ref, counts_ref, seq, block):
    base = block * WINDOW_LENGTH
    query = base + lax.broadcasted_iota(jnp.int32, (8, LANES), 1)
    oldest = jnp.zeros((8, LANES), jnp.int32)
    for entry in range(starts_ref.shape[1]):
        start = starts_ref[seq, entry]
        oldest = jnp.maximum(oldest, jnp.where(start <= query, start, 0))
    oldest = jnp.broadcast_to(oldest[:1], (WINDOW_LENGTH, LANES))
    key_row = lax.broadcasted_iota(jnp.int32, (WINDOW_LENGTH, LANES), 0)
    lower = lower_triangle()
    own_limit = counts_ref[seq, block]
    prev_limit = counts_ref[seq, jnp.maximum(block - 1, 0)]
    own = lower & (key_row + base >= oldest) & (key_row < own_limit)
    prev = (
        jnp.logical_not(lower)
        & (key_row + (base - WINDOW_LENGTH) >= oldest)
        & (key_row < prev_limit)
    )
    return jnp.where(own, 0.0, masked_score), jnp.where(prev, 0.0, masked_score)


class Shape:
    def __init__(self, seqs, heads_kv, group):
        self.seqs, self.heads_kv, self.group = seqs, heads_kv, group
        self.quads = group // 4
        self.tiles = heads_kv * group // 2

    def cat(self, ref, seq, head_kv, quads):
        first = head_kv * self.group // 2 + quads.start * 2
        count = 2 * len(quads)
        return ref[seq, first : first + count].reshape(count * WINDOW_LENGTH, LANES)

    def kv_tile(self, ref, seq, head_kv):
        at = head_kv // 2 * LANES
        return ref[seq, :, at : at + LANES]


def pack_kernel(k_ref, v_ref, out_ref, sems):
    copies = [
        pltpu.make_async_copy(ref, out_ref.at[kind], sems.at[kind])
        for kind, ref in enumerate((k_ref, v_ref))
    ]
    for copy in copies:
        copy.start()
    for copy in copies:
        copy.wait()


def own_kernel(
    sinks_hbm,
    starts_hbm,
    counts_hbm,
    q_hbm,
    g_hbm,
    kv_ref,
    q_ref,
    g_ref,
    s_ref,
    dp_ref,
    bias_ref,
    sink_ref,
    sinks_ref,
    starts_ref,
    counts_ref,
    small_sems,
    sems,
    *,
    shape,
):
    scaling = HEAD_DIMENSION**-0.5
    block = lax.axis_index("ctx")
    small = [
        pltpu.make_async_copy(source, target, small_sems.at[i])
        for i, (source, target) in enumerate(
            ((starts_hbm, starts_ref), (counts_hbm, counts_ref), (sinks_hbm, sinks_ref))
        )
    ]
    for copy in small:
        copy.start()
    copies = {}
    for seq in range(shape.seqs):
        for tile in range(shape.tiles):
            for kind, (source, target) in enumerate(((q_hbm, q_ref), (g_hbm, g_ref))):
                copy = pltpu.make_async_copy(
                    source.at[seq, :, tile * LANES : (tile + 1) * LANES],
                    target.at[seq, tile],
                    sems.at[seq, tile, kind],
                )
                copy.start()
                copies[seq, tile, kind] = copy
    for copy in small:
        copy.wait()
    for head in range(sink_ref.shape[0]):
        sink_ref[head : head + 1, :] = jnp.full((1, LANES), sinks_ref[head] / scaling, jnp.float32)
    for seq in range(shape.seqs):
        own, prev = biases(starts_ref, counts_ref, seq, block)
        bias_ref[seq] = prev
        own = twice(own)
        own = jnp.concatenate([own, own], axis=0)
        for head_kv in range(shape.heads_kv):
            keys = half_pair(shape.kv_tile(kv_ref.at[0], seq, head_kv), head_kv % 2)
            vals = half_pair(shape.kv_tile(kv_ref.at[1], seq, head_kv), head_kv % 2)
            for quad in range(shape.quads):
                at = head_kv * shape.group // 2 + quad * 2
                for kind in range(2):
                    for tile in (at, at + 1):
                        copies[seq, tile, kind].wait()
                some = range(quad, quad + 1)
                s_ref[seq, head_kv, quad] = dot_nt(keys, shape.cat(q_ref, seq, head_kv, some)) + own
                dp_ref[seq, head_kv, quad] = dot_nt(vals, shape.cat(g_ref, seq, head_kv, some))


def softmax_kernel(
    sinks_ref, q_ref, g_ref, halo_ref, s_ref, dp_ref, bias_ref, p_ref, ds_ref, sink_ref, sink_rows, *, shape
):
    scaling = HEAD_DIMENSION**-0.5
    to_exp2 = scaling * math.log2(math.e)
    lower = twice(lower_triangle())
    sink_rows[...] = jnp.zeros_like(sink_rows)
    for seq in range(shape.seqs):
        bias = twice(bias_ref[seq])
        for head_kv in range(shape.heads_kv):
            keys = half_pair(shape.kv_tile(halo_ref.at[0], seq, head_kv), head_kv % 2)
            vals = half_pair(shape.kv_tile(halo_ref.at[1], seq, head_kv), head_kv % 2)
            for quad in range(shape.quads):
                some = range(quad, quad + 1)
                scores = dot_nt(keys, shape.cat(q_ref, seq, head_kv, some))
                dprobs = dot_nt(vals, shape.cat(g_ref, seq, head_kv, some))
                for half in range(2):
                    rows = slice(half * WINDOW_LENGTH, (half + 1) * WINDOW_LENGTH)
                    head = head_kv * shape.group + quad * 4 + half
                    sink = jnp.concatenate(
                        [sinks_ref[head : head + 1, :], sinks_ref[head + 2 : head + 3, :]], axis=1
                    )
                    s = jnp.maximum(s_ref[seq, head_kv, quad, rows], scores[rows] + bias)
                    top = jnp.maximum(jnp.max(s, axis=0, keepdims=True), sink)
                    power = jnp.exp2((s - top) * to_exp2)
                    sink_power = jnp.exp2((sink - top) * to_exp2)
                    inverse = 1.0 / (jnp.sum(power, axis=0, keepdims=True) + sink_power)
                    dprob = jnp.where(lower, dp_ref[seq, head_kv, quad, rows], dprobs[rows])
                    delta = jnp.sum(power * dprob, axis=0, keepdims=True) * inverse
                    prob = power * inverse
                    p_ref[seq, head_kv, quad, rows] = prob.astype(jnp.bfloat16)
                    ds_ref[seq, head_kv, quad, rows] = (prob * (dprob - delta)).astype(jnp.bfloat16)
                    sink_term = sink_power * inverse * delta
                    sink_rows[head : head + 1, :] += sink_term[:, :LANES]
                    sink_rows[head + 2 : head + 3, :] += sink_term[:, LANES:]
    sink_ref[...] = -jnp.sum(sink_rows[...].T, axis=0, keepdims=True)


def kv_grad_kernel(q_ref, g_ref, p_ref, ds_ref, out_ref, *, shape, own):
    scaling = HEAD_DIMENSION**-0.5
    lower = twice(lower_triangle())
    keep = jnp.where(lower, 1.0 if own else 0.0, 0.0 if own else 1.0).astype(jnp.bfloat16)
    low = lane_half(WINDOW_LENGTH)
    for seq in range(shape.seqs):
        for kind, (weight_ref, wide_ref, factor) in enumerate(
            ((ds_ref, q_ref, scaling), (p_ref, g_ref, 1.0))
        ):
            for pair in range(shape.heads_kv // 2):
                sums = []
                for head_kv in (2 * pair, 2 * pair + 1):
                    right = shape.cat(wide_ref, seq, head_kv, range(shape.quads))
                    left = jnp.concatenate(
                        [
                            jnp.concatenate(
                                [
                                    weight_ref[
                                        seq, head_kv, quad, half * WINDOW_LENGTH : (half + 1) * WINDOW_LENGTH
                                    ]
                                    * keep
                                    for quad in range(shape.quads)
                                ],
                                axis=1,
                            )
                            for half in range(2)
                        ],
                        axis=0,
                    )
                    both = dot_nn(left, right)
                    sums.append((both[:WINDOW_LENGTH], both[WINDOW_LENGTH:]))
                (lo0, hi0), (lo1, hi1) = sums
                grad = jnp.where(low, lo0, hi1) + pltpu.roll(
                    jnp.where(low, lo1, hi0), HEAD_DIMENSION, 1
                )
                out_ref[kind, seq, :, pair * LANES : (pair + 1) * LANES] = (grad * factor).astype(
                    out_ref.dtype
                )


def query_grad_kernel(kv_ref, halo_ref, ds_ref, dq_ref, *, shape):
    scaling = HEAD_DIMENSION**-0.5
    lower_low = jnp.where(twice(lower_triangle()), 1.0, 0.0).astype(jnp.bfloat16)
    for seq in range(shape.seqs):
        for head_kv in range(shape.heads_kv):
            rows = slice(head_kv % 2 * HEAD_DIMENSION, (head_kv % 2 + 1) * HEAD_DIMENSION)
            keys_t = jnp.concatenate(
                [
                    shape.kv_tile(kv_ref.at[0], seq, head_kv).T[rows],
                    shape.kv_tile(halo_ref.at[0], seq, head_kv).T[rows],
                ],
                axis=1,
            )
            for quad in range(shape.quads):
                parts = []
                for half in range(2):
                    dscore = ds_ref[
                        seq, head_kv, quad, half * WINDOW_LENGTH : (half + 1) * WINDOW_LENGTH
                    ]
                    own = dscore * lower_low
                    parts.append(
                        dot_nn(keys_t, jnp.concatenate([own, dscore - own], axis=0)) * scaling
                    )
                for part in range(2):
                    lanes = slice(part * LANES, (part + 1) * LANES)
                    at = (head_kv * shape.group // 2 + quad * 2 + part) * LANES
                    tile = jnp.concatenate([parts[0][:, lanes], parts[1][:, lanes]], axis=0)
                    dq_ref[seq, :, at : at + LANES] = tile.astype(jnp.bfloat16).T


def add_kernel(own_ref, edge_ref, dk_ref, dv_ref):
    dk_ref[...] = (own_ref[0] + edge_ref[0].astype(jnp.float32)).astype(jnp.bfloat16)
    dv_ref[...] = (own_ref[1] + edge_ref[1].astype(jnp.float32)).astype(jnp.bfloat16)


VMEM = pl.BlockSpec(memory_space=pltpu.VMEM)
HBM = pl.BlockSpec(memory_space=pltpu.HBM)


def in_hbm(value):
    return pltpu.with_memory_space_constraint(value, pltpu.HBM)


def call(kernel, in_specs, outs, flops, scratch=(), **settings):
    return pl.pallas_call(
        functools.partial(kernel, **settings),
        in_specs=in_specs,
        out_specs=jax.tree.map(lambda _: VMEM, outs),
        out_shape=outs,
        scratch_shapes=scratch,
        cost_estimate=pl.CostEstimate(flops=flops, transcendentals=0, bytes_accessed=1024),
        compiler_params=pltpu.CompilerParams(vmem_limit_bytes=24 * 2**20),
        name=kernel.__name__,
    )


def local(queries, keys, values, output_gradient, sinks, doc_starts, valid_counts):
    seq_count, row_count, query_width = queries.shape
    kv_width = keys.shape[2]
    heads_kv = kv_width // HEAD_DIMENSION
    head_count = sinks.shape[0]
    shape = Shape(seq_count, heads_kv, head_count // heads_kv)
    assert row_count == WINDOW_LENGTH
    product = 2 * seq_count * head_count * WINDOW_LENGTH * WINDOW_LENGTH * HEAD_DIMENSION
    tiles = (seq_count, heads_kv, shape.quads, 2 * WINDOW_LENGTH, 2 * LANES)
    padded_heads = -(-head_count // LANES) * LANES
    f32, bf16 = jnp.float32, jnp.bfloat16
    new = jax.ShapeDtypeStruct

    both = call(
        pack_kernel,
        [HBM] * 2,
        new((2,) + keys.shape, bf16),
        product // 8,
        scratch=[pltpu.SemaphoreType.DMA((2,))],
    )(in_hbm(keys), in_hbm(values))
    halo = passed_along(both, "ctx", 1)
    wide_tiles = (seq_count, shape.tiles, WINDOW_LENGTH, LANES)
    q_tiles, g_tiles, scores, dprobs, bias, sink_lanes = call(
        own_kernel,
        [HBM] * 5 + [VMEM],
        [
            new(wide_tiles, bf16),
            new(wide_tiles, bf16),
            new(tiles, f32),
            new(tiles, f32),
            new((seq_count, WINDOW_LENGTH, LANES), f32),
            new((head_count, LANES), f32),
        ],
        2 * product,
        scratch=[
            pltpu.SMEM(sinks.shape, f32),
            pltpu.SMEM(doc_starts.shape, jnp.int32),
            pltpu.SMEM(valid_counts.shape, jnp.int32),
            pltpu.SemaphoreType.DMA((3,)),
            pltpu.SemaphoreType.DMA((seq_count, shape.tiles, 2)),
        ],
        shape=shape,
    )(*map(in_hbm, (sinks, doc_starts, valid_counts, queries, output_gradient)), both)
    prob, dscore, sink_part = call(
        softmax_kernel,
        [VMEM] * 7,
        [new(tiles, bf16), new(tiles, bf16), new((1, padded_heads), f32)],
        2 * product,
        scratch=[pltpu.VMEM((padded_heads, LANES), f32)],
        shape=shape,
    )(sink_lanes, q_tiles, g_tiles, halo, scores, dprobs, bias)
    prev = call(
        kv_grad_kernel, [VMEM] * 4, new((2,) + keys.shape, bf16), 2 * product, shape=shape, own=False
    )(q_tiles, g_tiles, prob, dscore)
    edge = passed_along(prev, "ctx", -1)
    query_grad = call(
        query_grad_kernel, [VMEM] * 3, new(queries.shape, bf16), 2 * product, shape=shape
    )(both, halo, dscore)
    own = call(
        kv_grad_kernel, [VMEM] * 4, new((2,) + keys.shape, f32), 2 * product, shape=shape, own=True
    )(q_tiles, g_tiles, prob, dscore)
    key_grad, value_grad = call(
        add_kernel, [VMEM] * 2, [new(keys.shape, bf16), new(keys.shape, bf16)], product // 8
    )(own, edge)
    sink_grad = total_over(sink_part, ("dp", "ctx"))[0, :head_count]
    return (query_grad, key_grad, value_grad, sink_grad)


def solution(mesh):
    placed = (
        P("dp", "ctx", "tp"),
        P("dp", "ctx", "tp"),
        P("dp", "ctx", "tp"),
        P("dp", "ctx", "tp"),
        P("tp"),
        P("dp", None),
        P("dp", None),
    )
    return jax.shard_map(
        local,
        mesh=mesh,
        in_specs=placed,
        out_specs=(P("dp", "ctx", "tp"), P("dp", "ctx", "tp"), P("dp", "ctx", "tp"), P("tp")),
        check_vma=False,
    )
```
